256 devices in a mesh: lev: 8 (over z), wav: 32 (over y, x, core).
Axes of the slice: x: 4, y: 4, z: 8, core: 2. Of those that a mesh axis runs over, the one named last changes fastest.
Arguments:
- grid_field: float32 [16, 1216, 1216], P('lev', 'wav'), may hold values from -6 to 6
- truncation_limit: int32 [1216], replicated, may hold values from -1 to 607, as said below
- diffusion_order: int32 [16], P('lev'), may hold values from 1 to 4
- diffusion_strength: float32 [16], P('lev'), may hold values from 2 to 50
- mass_weight: float32 [16], P('lev'), may hold values from 0.25 to 4
Outputs:
- filtered: float32 [16, 1216, 1216], P('lev', 'wav')
- energies: float32 [16], P('lev')
- total_energy: float32 [], replicated
The draws below stay inside these ranges and needn't reach their ends.
Inputs may be any that keep to these rules, and one draw needn't show every extreme that they name: `truncation_limit`: the largest |wavenumber(q)| kept at index p, with wavenumber(m) = m below 608 and m - 1216 otherwise; the kept set is an ellipse about wavenumber zero; the value at p equals the value at 1216 - p; -1 where nothing is kept; the value at p = 0 is 607.
All inputs are finite; a program needn't handle non-finite values.
Results may differ from the reference program's by a relative error of at most 0.000071.
Values sent between devices are 32-bit elements.
A program may use at most 64 MiB of HBM per device.

```python
import math
import jax
import jax.numpy as jnp
from jax import lax

N = 1216
SLABS = 16


def draw_truncation_limit(key, part):
    axis_second = jax.random.randint(key, (), 3 * N // 10, N // 2)
    axis_first = N // 2 - 1
    positions = jnp.arange(N, dtype=jnp.int32)
    distance = jnp.abs(jnp.where(positions < N // 2, positions, positions - N))
    steps_first = jnp.arange(N // 2 + 1, dtype=jnp.int32)
    scaled_second = distance * 1000 // axis_second
    scaled_first = steps_first * 1000 // axis_first
    inside = scaled_second[:, None] ** 2 + scaled_first[None, :] ** 2 <= 1000000
    return (jnp.sum(inside.astype(jnp.int32), axis=1) - 1).astype(jnp.int32)


def set_ends(drawn, key, smallest, largest):
    place = [jax.random.randint(jax.random.fold_in(key, axis), (), 0, length) for axis, length in enumerate(drawn.shape)]
    longest = drawn.shape.index(max(drawn.shape))
    neighbour = place[:longest] + [(place[longest] + 1) % drawn.shape[longest]] + place[longest + 1:]
    return drawn.at[tuple(place)].set(smallest).at[tuple(neighbour)].set(largest)


def block_levels(key, extent, pieces, low, largest):
    loudness, own = 1.0, jax.random.fold_in(key, 6)
    for position, shards_of in pieces:
        draws = jnp.exp(jax.random.uniform(jax.random.fold_in(own, position), (shards_of,), jnp.float32, low / len(pieces), largest / len(pieces)))
        loudness = loudness * jnp.repeat(draws, extent[position] // shards_of).reshape([-1 if axis == position else 1 for axis in range(len(extent))])
    return loudness


def centred(own_key, extent, spread, bound, split=(), kind=jnp.bfloat16):
    gain = block_levels(own_key, extent, split, -0.22, 0.18) if split else 1.0
    drawn = jax.random.normal(own_key, extent, jnp.float32) * spread * gain
    return jnp.minimum(jnp.maximum(drawn, -bound), bound).astype(kind)


def setup_inputs(seed: int = 0) -> dict:
    key_list = jax.random.split(jax.random.key(seed), 6)
    grid_field = centred(key_list[0], (SLABS, N, N), 1.0, 6.0, ((0, 8), (1, 32)), jnp.float32)
    truncation_limit = draw_truncation_limit(jax.random.fold_in(key_list[5], 71), 0)
    diffusion_order = set_ends(jax.random.randint(key_list[2], (SLABS,), 1, 5), jax.random.fold_in(key_list[2], 1), 1, 4).astype(jnp.int32)
    diffusion_strength = jnp.clip(jnp.exp(math.log(50.0) - 3.218876 * jax.random.uniform(key_list[3], (SLABS,), jnp.float32) ** block_levels(key_list[3], (SLABS,), ((0, 8),), -0.2, 0.2)), 2.0, 50.0)
    mass_weight = jnp.clip(jnp.exp(math.log(4.0) - 2.7725887 * jax.random.uniform(key_list[4], (SLABS,), jnp.float32) ** block_levels(key_list[4], (SLABS,), ((0, 8),), -0.2, 0.2)), 0.25, 4.0)
    return dict(grid_field=grid_field, truncation_limit=truncation_limit, diffusion_order=diffusion_order, diffusion_strength=diffusion_strength, mass_weight=mass_weight)


def signed(positions, length):
    return jnp.where(positions < length // 2, positions, positions - length)


def reference(grid_field, truncation_limit, diffusion_order, diffusion_strength, mass_weight):
    positions = jnp.arange(N, dtype=jnp.int32)
    signed_index = signed(positions, N)
    wavenumber = signed_index.astype(jnp.float32)
    scaled_radius = (wavenumber[:, None] ** 2 + wavenumber[None, :] ** 2) / (0.5 * N) ** 2
    inside = (jnp.abs(signed_index)[None, :] <= truncation_limit[:, None]).astype(jnp.float32)

    def one_slab(members):
        slab_field, degree, strength = members
        spectrum = jnp.fft.fft2(slab_field).T
        damping = inside / (1.0 + strength * jnp.power(scaled_radius, degree.astype(jnp.float32)))
        damped = spectrum * damping
        energy = jnp.sum(jnp.real(damped) ** 2 + jnp.imag(damped) ** 2) / float(N) ** 4
        filtered = jnp.real(jnp.fft.ifft2(damped.T))
        return filtered, energy

    filtered, energies = lax.map(one_slab, (grid_field, diffusion_order, diffusion_strength))
    total_energy = jnp.sum(mass_weight * energies) / SLABS
    return filtered, energies, total_energy
```

```python
import math

import jax
import jax.numpy as jnp
import numpy as np
from jax import lax
from jax.experimental import pallas as pl
from jax.experimental.pallas import tpu as pltpu
from jax.sharding import PartitionSpec as P

MESH = pl.DeviceIdType.MESH
f32, bf16 = jnp.float32, jnp.bfloat16

LENGTH = 1216
HALF = LENGTH // 2
PAD = 640
ROWS = 38
PITCH = 40
GROUP = 76
PEERS = 32


def basis(parity):
    index = np.arange(HALF, dtype=np.int64)
    if parity == 0:
        phase = (index[:, None] * index[None, :]) % HALF
        angle = phase.astype(np.float64) * (2.0 * math.pi / HALF)
    else:
        phase = ((2 * index[:, None] + 1) * (2 * index[None, :] + 1)) % (4 * HALF)
        angle = phase.astype(np.float64) * (2.0 * math.pi / (4 * HALF))
    table = np.zeros((HALF, PAD), np.float32)
    table[:, :HALF] = np.cos(angle) + np.sin(angle)
    high = table.astype(bf16)
    low = (table - high.astype(np.float32)).astype(bf16)
    return high, low


def dot(a, b):
    return jnp.dot(a, b, preferred_element_type=f32)


def split(values):
    high = values.astype(bf16)
    return high, (values - high.astype(f32)).astype(bf16)


def lanes(shape):
    return lax.broadcasted_iota(jnp.int32, shape, len(shape) - 1)


def pack(block):
    third, fourth = block[24:32], block[32:40]
    lane = lanes((8, 128))
    tail = [
        pltpu.roll(third, 76, 1),
        pltpu.roll(fourth, 76, 1),
        jnp.where(lane < 100, pltpu.roll(third, 24, 1), pltpu.roll(fourth, 48, 1)),
    ]
    return [jnp.where(lane < GROUP, block[8 * i : 8 * i + 8], tail[i]) for i in range(3)]


def unpack(first, second, third):
    lane = lanes((8, 128))
    return [
        first,
        second,
        third,
        jnp.where(lane < 52, pltpu.roll(first, 52, 1), pltpu.roll(third, 104, 1)),
        jnp.where(lane < 52, pltpu.roll(second, 52, 1), pltpu.roll(third, 80, 1)),
    ]


def chip_of(parity, group):
    return (group // 2) * 4 + (group % 2) * 2 + parity


def kernel(
    x_ref, limit_ref, order_ref, strength_ref, mass_ref, eh_hbm, el_hbm, oh_hbm, ol_hbm,
    out_ref, energy_ref, total_ref,
    tables, xs, ybuf, wbuf, gbuf, damp,
    send1, recv1, send2, recv2, esend, erecv, lsend, lrecv,
    table_sem, s1, r1, s2, r2, es, er, ls, lr,
):
    lev = lax.axis_index("lev")
    me = lax.axis_index("wav")
    core = me % 2
    chip_x = (me // 2) % 4
    parity_me = chip_x % 2
    group_me = (me // 8) * 2 + chip_x // 2

    loads = [
        pltpu.make_async_copy(source, tables.at[i, pl.ds(0, HALF)], table_sem.at[i])
        for i, source in enumerate((eh_hbm, el_hbm, oh_hbm, ol_hbm))
    ]
    for load in loads:
        load.start()

    barrier = pltpu.get_barrier_semaphore()

    def greet(k, carry):
        pl.semaphore_signal(barrier, inc=1, device_id=(lev, (me + k) % PEERS), device_id_type=MESH)
        return carry

    def greet_lev(k, carry):
        pl.semaphore_signal(barrier, inc=1, device_id=((lev + k) % 8, me), device_id_type=MESH)
        return carry

    lax.fori_loop(1, PEERS, greet, 0)
    lax.fori_loop(1, 8, greet_lev, 0)

    tables[:, HALF:, :] = jnp.zeros((4, PAD - HALF, PAD), bf16)
    xs[:, 32:40, :] = jnp.zeros((2, 8, 1280), f32)
    xs[:, :, 1152:] = jnp.zeros((2, 40, 128), f32)
    for s in range(2):
        xs[s, :ROWS, :LENGTH] = x_ref[s]
    lane640 = lanes((PITCH, PAD))
    folded = [[], []]
    for s in range(2):
        whole = xs[s]
        lower = jnp.where(lane640 < HALF, whole[:, :PAD], 0.0)
        upper = pltpu.roll(whole, 1280 - HALF, 1)[:, :PAD]
        folded[0].append(lower + upper)
        folded[1].append(lower - upper)

    def spread(parity):
        for g in range(8):
            tile, offset = divmod(GROUP * g, 128)
            lane = lanes((80, 128))
            piece = ybuf[:, 128 * tile : 128 * tile + 128]
            if offset:
                piece = pltpu.roll(piece, 128 - offset, 1)
            if offset + GROUP > 128:
                after = pltpu.roll(ybuf[:, 128 * tile + 128 : 128 * tile + 256], 128 - offset, 1)
                piece = jnp.where(lane < 128 - offset, piece, after)
            for c in range(2):
                packed = pack(piece[PITCH * c : PITCH * c + PITCH])
                e = chip_of(parity, g) * 2 + c
                for i in range(3):
                    send1[e, 8 * i : 8 * i + 8, :] = packed[i]

    def exchange(send, recv, ssem, rsem, e):
        return pltpu.make_async_remote_copy(
            src_ref=send.at[e], dst_ref=recv.at[me], send_sem=ssem.at[e], recv_sem=rsem.at[me],
            device_id=(lev, e), device_id_type=MESH,
        )

    def await_from(send, recv, ssem, rsem, e):
        pltpu.make_async_remote_copy(
            src_ref=send.at[e], dst_ref=recv.at[e], send_sem=ssem.at[e], recv_sem=rsem.at[e],
            device_id=(lev, e), device_id_type=MESH,
        ).wait_recv()

    def await_sent(send, recv, ssem, rsem, e):
        exchange(send, recv, ssem, rsem, e).wait_send()

    first_copy = (send1, recv1, s1, r1)
    second_copy = (send2, recv2, s2, r2)
    energy_copy = (esend, erecv, es, er)

    def over_peers(body):
        def step(k, carry):
            body((me + k) % PEERS)
            return carry

        lax.fori_loop(1, PEERS, step, 0)

    for parity in range(2):
        high, low = split(jnp.concatenate(folded[parity], axis=0))
        loads[2 * parity].wait()
        loads[2 * parity + 1].wait()
        both = dot(jnp.concatenate([high, low], axis=0), tables[2 * parity])
        ybuf[...] = both[:80] + both[80:] + dot(high, tables[2 * parity + 1])
        spread(parity)
    pl.semaphore_wait(barrier, PEERS - 1 + 7)
    over_peers(lambda e: exchange(*first_copy, e).start())
    recv1[me] = send1[me]

    order = order_ref[core]
    strength = strength_ref[core]

    def place(l, carry):
        value = limit_ref[2 * (GROUP * group_me + l) + parity_me]
        return jnp.where(lanes((8, 128)) == l, value, carry)

    limits = lax.fori_loop(0, GROUP, place, jnp.full((8, 128), -1, jnp.int32))[:1]
    lane1 = lanes((1, 128))
    index1 = GROUP * group_me + lane1
    twice1 = 2 * index1 + parity_me
    wave1 = jnp.minimum(twice1, LENGTH - twice1).astype(f32)
    index2 = lax.broadcasted_iota(jnp.int32, (PAD, 128), 0)
    for parity in range(2):
        twice2 = 2 * index2 + parity
        wave2 = jnp.minimum(twice2, LENGTH - twice2)
        first = wave2.astype(f32)
        radius = (wave1 * wave1 + first * first) / float(HALF) ** 2
        square = radius * radius
        powered = jnp.where(order >= 2, square, radius)
        powered = jnp.where(order >= 3, square * radius, powered)
        powered = jnp.where(order >= 4, square * square, powered)
        kept = (wave2 <= limits) & (lane1 < GROUP) & (index2 < HALF)
        damp[parity] = jnp.where(
            kept, (1.0 / float(LENGTH) ** 2) / (1.0 + strength * powered), 0.0
        )

    wbuf[:, HALF:, :] = jnp.zeros((2, PAD - HALF, 128), f32)
    over_peers(lambda e: await_from(*first_copy, e))
    for d in range(16):
        sums = [recv1[d, 8 * i : 8 * i + 8] + recv1[d + 16, 8 * i : 8 * i + 8] for i in range(3)]
        differences = [recv1[d, 8 * i : 8 * i + 8] - recv1[d + 16, 8 * i : 8 * i + 8] for i in range(3)]
        for parity, packed in enumerate((sums, differences)):
            pieces = unpack(*packed)
            for i in range(5):
                count = 8 if i < 4 else ROWS - 32
                start = ROWS * d + 8 * i
                wbuf[parity, start : start + count, :] = pieces[i][:count]
    energy = jnp.zeros((8, 128), f32)
    spectra = []
    for parity in range(2):
        high, low = split(wbuf[parity])
        both = dot(tables[2 * parity], jnp.concatenate([high, low], axis=1))
        spectrum = both[:, :128] + both[:, 128:] + dot(tables[2 * parity + 1], high)
        damped = spectrum * damp[parity]
        energy = energy + jnp.sum((damped * damped).reshape(PAD // 8, 8, 128), axis=0)
        high, low = split(damped)
        spectra.append(jnp.concatenate([high, low], axis=1))
    partial_value = jnp.full((8, 128), jnp.sum(energy))
    esend[...] = partial_value

    def energy_to(e):
        return pltpu.make_async_remote_copy(
            src_ref=esend, dst_ref=erecv.at[me], send_sem=es.at[e], recv_sem=er.at[me],
            device_id=(lev, e), device_id_type=MESH,
        )

    def energy_from(e):
        return pltpu.make_async_remote_copy(
            src_ref=esend, dst_ref=erecv.at[e], send_sem=es.at[e], recv_sem=er.at[e],
            device_id=(lev, e), device_id_type=MESH,
        )

    def level_to(e):
        return pltpu.make_async_remote_copy(
            src_ref=lsend, dst_ref=lrecv.at[lev], send_sem=ls.at[e], recv_sem=lr.at[lev],
            device_id=(e, me), device_id_type=MESH,
        )

    def level_from(e):
        return pltpu.make_async_remote_copy(
            src_ref=lsend, dst_ref=lrecv.at[e], send_sem=ls.at[e], recv_sem=lr.at[e],
            device_id=(e, me), device_id_type=MESH,
        )

    over_peers(lambda e: energy_to(e).start())
    erecv[me] = partial_value

    for part in range(2):
        rows = slice(304 * part, 304 * part + 304)
        for parity in range(2):
            both = dot(tables[2 * parity, rows], spectra[parity])
            gbuf[parity, rows] = (
                both[:, :128] + both[:, 128:]
                + dot(tables[2 * parity + 1, rows], spectra[parity][:, :128])
            )
        if part == 1:
            gbuf[:, HALF:] = jnp.zeros((2, PAD - HALF, 128), f32)
        for d in range(8 * part, 8 * part + 8):
            count = PITCH if d % 8 < 7 or part == 1 else ROWS
            even = gbuf[0, ROWS * d : ROWS * d + count]
            odd = gbuf[1, ROWS * d : ROWS * d + count]
            if count < PITCH:
                even = jnp.concatenate([even, jnp.zeros((PITCH - count, 128), f32)], axis=0)
                odd = jnp.concatenate([odd, jnp.zeros((PITCH - count, 128), f32)], axis=0)
            for e, block in ((d, even + odd), (d + 16, even - odd)):
                packed = pack(block)
                for i in range(3):
                    send2[e, 8 * i : 8 * i + 8, :] = packed[i]
    over_peers(lambda e: exchange(*second_copy, e).start())
    recv2[me] = send2[me]

    over_peers(lambda e: energy_from(e).wait_recv())
    sums = [erecv[0], erecv[1]]
    for e in range(2, PEERS):
        sums[e % 2] = sums[e % 2] + erecv[e]
    weighted = mass_ref[0] * sums[0] + mass_ref[1] * sums[1]
    lsend[...] = weighted
    energy_ref[0] = sums[0][0, 0]
    energy_ref[1] = sums[1][0, 0]

    def over_levels(body):
        def step(k, carry):
            body((lev + k) % 8)
            return carry

        lax.fori_loop(1, 8, step, 0)

    over_levels(lambda e: level_to(e).start())
    lrecv[lev] = weighted

    over_peers(lambda e: await_from(*second_copy, e))
    results = []
    for parity in range(2):
        halves = []
        for c in range(2):
            tiles = [None] * 5
            for g in range(8):
                e = chip_of(parity, g) * 2 + c
                pieces = unpack(*[recv2[e, 8 * i : 8 * i + 8] for i in range(3)])
                tile, offset = divmod(GROUP * g, 128)
                block = jnp.concatenate(pieces, axis=0)
                if offset:
                    block = pltpu.roll(block, offset, 1)
                lane = lanes((PITCH, 128))
                if tiles[tile] is None:
                    tiles[tile] = block
                else:
                    tiles[tile] = jnp.where(lane < offset, tiles[tile], block)
                if offset + GROUP > 128:
                    tiles[tile + 1] = block
            tiles[4] = jnp.where(lanes((PITCH, 128)) < HALF - 512, tiles[4], 0.0)
            halves.append(jnp.concatenate(tiles, axis=1))
        high, low = split(jnp.concatenate(halves, axis=0))
        both = dot(jnp.concatenate([high, low], axis=0), tables[2 * parity])
        results.append(both[:80] + both[80:] + dot(high, tables[2 * parity + 1]))
    sums = results[0] + results[1]
    differences = results[0] - results[1]
    blank = jnp.zeros((80, PAD), f32)
    whole = jnp.concatenate([sums, blank], axis=1) + pltpu.roll(
        jnp.concatenate([differences, blank], axis=1), HALF, 1
    )
    for s in range(2):
        out_ref[s] = whole[PITCH * s : PITCH * s + ROWS, :LENGTH]

    over_levels(lambda e: level_from(e).wait_recv())
    total = lrecv[0]
    for e in range(1, 8):
        total = total + lrecv[e]
    total_ref[0] = total[0, 0] / 16.0

    over_peers(lambda e: await_sent(*first_copy, e))
    over_peers(lambda e: energy_to(e).wait_send())
    over_peers(lambda e: await_sent(*second_copy, e))
    over_levels(lambda e: level_to(e).wait_send())


def local(grid_field, truncation_limit, diffusion_order, diffusion_strength, mass_weight):
    table_list = [jnp.asarray(t) for parity in range(2) for t in basis(parity)]
    vmem = pl.BlockSpec(memory_space=pltpu.VMEM)
    smem = pl.BlockSpec(memory_space=pltpu.SMEM)
    anywhere = pl.BlockSpec(memory_space=pl.ANY)
    dma = pltpu.SemaphoreType.DMA
    filtered, energies, total = pl.pallas_call(
        kernel,
        out_shape=(
            jax.ShapeDtypeStruct(grid_field.shape, f32),
            jax.ShapeDtypeStruct((2,), f32),
            jax.ShapeDtypeStruct((1,), f32),
        ),
        in_specs=[vmem, smem, smem, smem, smem] + [anywhere] * 4,
        out_specs=(vmem, smem, smem),
        scratch_shapes=[
            pltpu.VMEM((4, PAD, PAD), bf16),
            pltpu.VMEM((2, PITCH, 1280), f32),
            pltpu.VMEM((80, PAD), f32),
            pltpu.VMEM((2, PAD, 128), f32),
            pltpu.VMEM((2, PAD, 128), f32),
            pltpu.VMEM((2, PAD, 128), f32),
            pltpu.VMEM((PEERS, 24, 128), f32),
            pltpu.VMEM((PEERS, 24, 128), f32),
            pltpu.VMEM((PEERS, 24, 128), f32),
            pltpu.VMEM((PEERS, 24, 128), f32),
            pltpu.VMEM((8, 128), f32),
            pltpu.VMEM((PEERS, 8, 128), f32),
            pltpu.VMEM((8, 128), f32),
            pltpu.VMEM((8, 8, 128), f32),
            dma((4,)),
            dma((PEERS,)), dma((PEERS,)), dma((PEERS,)), dma((PEERS,)),
            dma((PEERS,)), dma((PEERS,)), dma((8,)), dma((8,)),
        ],
        compiler_params=pltpu.CompilerParams(
            collective_id=0, has_side_effects=True, vmem_limit_bytes=48 * 1024 * 1024
        ),
    )(grid_field, truncation_limit, diffusion_order, diffusion_strength, mass_weight, *table_list)
    return filtered, energies, total.reshape(())


def solution(mesh):
    placed = (P("lev", "wav", None), P(), P("lev"), P("lev"), P("lev"))
    return jax.shard_map(
        local,
        mesh=mesh,
        in_specs=placed,
        out_specs=(P("lev", "wav", None), P("lev"), P()),
        check_vma=False,
    )
```

```python
import math

import jax
import jax.numpy as jnp
import numpy as np
from jax import lax
from jax.experimental import pallas as pl
from jax.experimental.pallas import tpu as pltpu
from jax.sharding import PartitionSpec as P

MESH = pl.DeviceIdType.MESH
f32, bf16 = jnp.float32, jnp.bfloat16

LENGTH = 1216
HALF = LENGTH // 2
PAD = 640
ROWS = 38
PITCH = 40
GROUP = 76
PEERS = 32


def basis(parity):
    index = np.arange(HALF, dtype=np.int64)
    if parity == 0:
        phase = (index[:, None] * index[None, :]) % HALF
        angle = phase.astype(np.float64) * (2.0 * math.pi / HALF)
    else:
        phase = ((2 * index[:, None] + 1) * (2 * index[None, :] + 1)) % (4 * HALF)
        angle = phase.astype(np.float64) * (2.0 * math.pi / (4 * HALF))
    table = np.zeros((HALF, PAD), np.float32)
    table[:, :HALF] = np.cos(angle) + np.sin(angle)
    high = table.astype(bf16)
    low = (table - high.astype(np.float32)).astype(bf16)
    return np.concatenate([high, low], axis=1)


def dot(a, b):
    return jnp.dot(a, b, preferred_element_type=f32)


def split(values):
    high = values.astype(bf16)
    return high, (values - high.astype(f32)).astype(bf16)


def lanes(shape):
    return lax.broadcasted_iota(jnp.int32, shape, len(shape) - 1)


def pack(block, extra=None):
    third, fourth = block[24:32], block[32:40]
    lane = lanes((8, 128))
    tail = [
        pltpu.roll(third, 76, 1),
        pltpu.roll(fourth, 76, 1),
        jnp.where(lane < 100, pltpu.roll(third, 24, 1), pltpu.roll(fourth, 48, 1)),
    ]
    if extra is not None:
        tail[2] = jnp.where(lane < 124, tail[2], extra)
    return [jnp.where(lane < GROUP, block[8 * i : 8 * i + 8], tail[i]) for i in range(3)]


def unpack(first, second, third):
    lane = lanes((8, 128))
    return [
        first,
        second,
        third,
        jnp.where(lane < 52, pltpu.roll(first, 52, 1), pltpu.roll(third, 104, 1)),
        jnp.where(lane < 52, pltpu.roll(second, 52, 1), pltpu.roll(third, 80, 1)),
    ]


def chip_of(parity, group):
    return (group // 2) * 4 + (group % 2) * 2 + parity


def kernel(
    x_ref, limit_ref, order_ref, strength_ref, mass_ref, even_hbm, odd_hbm,
    out_ref, value_ref,
    limit, order_all, strength_all, mass, xin, tables, xs, ybuf, wbuf, gbuf, damp,
    send1, recv1, send2, recv2, esend, erecv, lsend, lrecv, tsend, trecv,
    x_sem, table_sem, small_sem, go, s1, r1, s2, r2, es, er, ls, lr, ts, tr,
):
    lev = lax.axis_index("lev")
    me = lax.axis_index("wav")
    core = me % 2
    chip_x = (me // 2) % 4
    chip_y = me // 8
    parity_me = chip_x % 2
    group_me = chip_y * 2 + chip_x // 2

    arrive = [pltpu.make_async_copy(x_ref.at[:, s], xin.at[s], x_sem.at[s]) for s in range(2)]
    loads = [
        pltpu.make_async_copy(source, tables.at[i, pl.ds(0, HALF)], table_sem.at[i])
        for i, source in enumerate((even_hbm, odd_hbm))
    ]
    small = [
        pltpu.make_async_copy(source, target, small_sem.at[i])
        for i, (source, target) in enumerate(
            ((limit_ref, limit), (order_ref, order_all), (strength_ref, strength_all), (mass_ref, mass))
        )
    ]
    for copy in arrive + loads + small:
        copy.start()

    barrier = pltpu.get_barrier_semaphore()

    def greet(k, carry):
        chip = (me // 2 + k) % 16
        pl.semaphore_signal(barrier, inc=1, device_id=(lev, chip * 2 + 1), device_id_type=MESH)
        return carry

    def greet_lev(k, carry):
        pl.semaphore_signal(barrier, inc=1, device_id=((lev + k) % 8, me), device_id_type=MESH)
        return carry

    lax.fori_loop(1, 16, greet, 0)

    @pl.when(core == 0)
    def _():
        greet(0, 0)
        lax.fori_loop(1, 8, greet_lev, 0)

    def enter():
        @pl.when(core == 1)
        def _():
            pl.semaphore_wait(barrier, PEERS - 1)
            pl.semaphore_signal(go, inc=1, device_id=(lev, me - 1), device_id_type=MESH)

        @pl.when(core == 0)
        def _():
            pl.semaphore_wait(go, 1)

    def exchange(send, recv, ssem, rsem, e):
        return pltpu.make_async_remote_copy(
            src_ref=send.at[e], dst_ref=recv.at[me], send_sem=ssem.at[e], recv_sem=rsem.at[me],
            device_id=(lev, e), device_id_type=MESH,
        )

    def await_from(send, recv, ssem, rsem, e):
        pltpu.make_async_remote_copy(
            src_ref=send.at[e], dst_ref=recv.at[e], send_sem=ssem.at[e], recv_sem=rsem.at[e],
            device_id=(lev, e), device_id_type=MESH,
        ).wait_recv()

    first_copy = (send1, recv1, s1, r1)
    second_copy = (send2, recv2, s2, r2)

    def over_peers(body):
        def step(k, carry):
            body((me + k) % PEERS)
            return carry

        lax.fori_loop(1, PEERS, step, 0)

    with jax.named_scope("t1_x"):
        tables[:, HALF:, :] = jnp.zeros((2, PAD - HALF, 2 * PAD), bf16)
        xs[:, 32:40, :] = jnp.zeros((2, 8, 1280), f32)
        xs[:, :, 1152:] = jnp.zeros((2, 40, 128), f32)
        for s in range(2):
            arrive[s].wait()
            xs[s, :ROWS, :LENGTH] = xin[s]
    lane640 = lanes((PITCH, PAD))
    folded = [[], []]
    for s in range(2):
        whole = xs[s]
        lower = jnp.where(lane640 < HALF, whole[:, :PAD], 0.0)
        upper = pltpu.roll(whole, 1280 - HALF, 1)[:, :PAD]
        folded[0].append(lower + upper)
        folded[1].append(lower - upper)

    def spread(parity):
        for g in range(8):
            tile, offset = divmod(GROUP * g, 128)
            lane = lanes((80, 128))
            piece = ybuf[:, 128 * tile : 128 * tile + 128]
            if offset:
                piece = pltpu.roll(piece, 128 - offset, 1)
            if offset + GROUP > 128:
                after = pltpu.roll(ybuf[:, 128 * tile + 128 : 128 * tile + 256], 128 - offset, 1)
                piece = jnp.where(lane < 128 - offset, piece, after)
            for c in range(2):
                packed = pack(piece[PITCH * c : PITCH * c + PITCH])
                e = chip_of(parity, g) * 2 + c
                for i in range(3):
                    send1[e, 8 * i : 8 * i + 8, :] = packed[i]

    def start_all(copy, peers):
        for e in peers[:-1]:
            exchange(*copy, e).start()

        @pl.when(peers[-1] != me)
        def _():
            exchange(*copy, peers[-1]).start()

    def column_peers(parity):
        return [
            ((chip_y + dy) % 4) * 8 + (parity + 2 * ((chip_x // 2 + j) % 2)) * 2 + (core + dc) % 2
            for dy in (2, 1, 3, 0) for j in (1, 0) for dc in (1, 0)
        ]

    def row_peers(parity):
        return [
            (parity + 2 * ((chip_y // 2 + j) % 2)) * 8 + ((chip_x + dx) % 4) * 2 + (core + dc) % 2
            for dx in (2, 1, 3, 0) for j in (1, 0) for dc in (1, 0)
        ]

    for parity in range(2):
        with jax.named_scope(f"t2_stage1_{parity}"):
            high, low = split(jnp.concatenate(folded[parity], axis=0))
            loads[parity].wait()
            both = dot(jnp.concatenate([high, low], axis=0), tables[parity, :, :PAD])
            ybuf[...] = both[:80] + both[80:] + dot(high, tables[parity, :, PAD:])
            spread(parity)
        if parity == 0:
            with jax.named_scope("t3_enter"):
                enter()
        with jax.named_scope(f"t4_send1_{parity}"):
            start_all(first_copy, column_peers(parity))
    recv1[me] = send1[me]

    with jax.named_scope("t5_damp"):
        for copy in small:
            copy.wait()
        order = order_all[core]
        strength = strength_all[core]

        def place(l, carry):
            value = limit[2 * (GROUP * group_me + l) + parity_me]
            return jnp.where(lanes((8, 128)) == l, value, carry)

        limits = lax.fori_loop(0, GROUP, place, jnp.full((8, 128), -1, jnp.int32))[:1]
        lane1 = lanes((1, 128))
        twice1 = 2 * (GROUP * group_me + lane1) + parity_me
        wave1 = jnp.minimum(twice1, LENGTH - twice1).astype(f32)
        index2 = lax.broadcasted_iota(jnp.int32, (PAD, 128), 0)
        for parity in range(2):
            twice2 = 2 * index2 + parity
            wave2 = jnp.minimum(twice2, LENGTH - twice2)
            first = wave2.astype(f32)
            radius = (wave1 * wave1 + first * first) / float(HALF) ** 2
            square = radius * radius
            powered = jnp.where(order >= 2, square, radius)
            powered = jnp.where(order >= 3, square * radius, powered)
            powered = jnp.where(order >= 4, square * square, powered)
            kept = (wave2 <= limits) & (lane1 < GROUP) & (index2 < HALF)
            damp[parity] = jnp.where(
                kept, (1.0 / float(LENGTH) ** 2) / (1.0 + strength * powered), 0.0
            )
        wbuf[:, HALF:, :] = jnp.zeros((2, PAD - HALF, 128), f32)
        gbuf[:, HALF:] = jnp.zeros((2, PAD - HALF, 128), f32)

    with jax.named_scope("t6_wait1"):
        over_peers(lambda e: await_from(*first_copy, e))
    with jax.named_scope("t7_stage2"):
        for d in range(16):
            near = [recv1[d, 8 * i : 8 * i + 8] for i in range(3)]
            far = [recv1[d + 16, 8 * i : 8 * i + 8] for i in range(3)]
            for parity in range(2):
                packed = [a + b if parity == 0 else a - b for a, b in zip(near, far)]
                pieces = unpack(*packed)
                for i in range(5):
                    count = 8 if i < 4 else ROWS - 32
                    start = ROWS * d + 8 * i
                    wbuf[parity, start : start + count, :] = pieces[i][:count]
        energy = jnp.zeros((8, 128), f32)
        blank = jnp.zeros((PAD, 128), bf16)

        def stacked(values):
            high, low = split(values)
            return jnp.concatenate(
                [jnp.concatenate([high, low], axis=1), jnp.concatenate([high, blank], axis=1)], axis=0
            )

        spectra = []
        for parity in range(2):
            both = dot(tables[parity], stacked(wbuf[parity]))
            damped = (both[:, :128] + both[:, 128:]) * damp[parity]
            energy = energy + jnp.sum((damped * damped).reshape(PAD // 8, 8, 128), axis=0)
            spectra.append(stacked(damped))
        partial_value = jnp.full((8, 128), jnp.sum(energy))
        esend[...] = mass[core] * partial_value

    def energy_to(e):
        return pltpu.make_async_remote_copy(
            src_ref=esend, dst_ref=erecv.at[me], send_sem=es.at[e // 2], recv_sem=er.at[me],
            device_id=(lev, e), device_id_type=MESH,
        )

    def energy_from(e):
        return pltpu.make_async_remote_copy(
            src_ref=esend, dst_ref=erecv.at[e], send_sem=es.at[0], recv_sem=er.at[e],
            device_id=(lev, e), device_id_type=MESH,
        )

    def level_to(e):
        return pltpu.make_async_remote_copy(
            src_ref=lsend, dst_ref=lrecv.at[lev], send_sem=ls.at[e], recv_sem=lr.at[lev],
            device_id=(e, me), device_id_type=MESH,
        )

    def level_from(e):
        return pltpu.make_async_remote_copy(
            src_ref=lsend, dst_ref=lrecv.at[e], send_sem=ls.at[e], recv_sem=lr.at[e],
            device_id=(e, me), device_id_type=MESH,
        )

    def total_to(e):
        return pltpu.make_async_remote_copy(
            src_ref=tsend, dst_ref=trecv, send_sem=ts, recv_sem=tr,
            device_id=(lev, e), device_id_type=MESH,
        )

    def over_heads(body, first):
        def step(k, carry):
            body(((me // 2 + k) % 16) * 2)
            return carry

        lax.fori_loop(first, 16, step, 0)

    def over_levels(body):
        def step(k, carry):
            body((lev + k) % 8)
            return carry

        lax.fori_loop(1, 8, step, 0)

    for part in range(2):
        with jax.named_scope(f"t8_stage3_{part}"):
            rows = slice(304 * part, 304 * part + 304)
            for parity in range(2):
                both = dot(tables[parity, rows], spectra[parity])
                gbuf[parity, rows] = both[:, :128] + both[:, 128:]
            for d in range(8 * part, 8 * part + 8):
                count = PITCH if d % 8 < 7 or part == 1 else ROWS
                even = gbuf[0, ROWS * d : ROWS * d + count]
                odd = gbuf[1, ROWS * d : ROWS * d + count]
                if count < PITCH:
                    even = jnp.concatenate([even, jnp.zeros((PITCH - count, 128), f32)], axis=0)
                    odd = jnp.concatenate([odd, jnp.zeros((PITCH - count, 128), f32)], axis=0)
                for e, block in ((d, even + odd), (d + 16, even - odd)):
                    packed = pack(block, partial_value)
                    for i in range(3):
                        send2[e, 8 * i : 8 * i + 8, :] = packed[i]
        if part == 0:
            with jax.named_scope("t9_esend"):
                over_heads(lambda e: energy_to(e).start(), 1)

                @pl.when(core == 1)
                def _():
                    energy_to(me - 1).start()

        with jax.named_scope(f"ta_send2_{part}"):
            start_all(second_copy, row_peers(part))
    recv2[me] = send2[me]

    with jax.named_scope("tb_energy"):
        @pl.when(core == 0)
        def _():
            erecv[me] = esend[...]
            over_peers(lambda e: energy_from(e).wait_recv())
            plane = erecv[0]
            for e in range(1, PEERS):
                plane = plane + erecv[e]
            lsend[...] = plane
            lrecv[lev] = plane
            pl.semaphore_wait(barrier, 7)
            over_levels(lambda e: level_to(e).start())

    with jax.named_scope("tc_wait2"):
        over_peers(lambda e: await_from(*second_copy, e))
    with jax.named_scope("td_stage4"):
        results = []
        for parity in range(2):
            halves = []
            for c in range(2):
                tiles = [None] * 5
                for g in range(8):
                    e = chip_of(parity, g) * 2 + c
                    pieces = unpack(*[recv2[e, 8 * i : 8 * i + 8] for i in range(3)])
                    tile, offset = divmod(GROUP * g, 128)
                    block = jnp.concatenate(pieces, axis=0)
                    if offset:
                        block = pltpu.roll(block, offset, 1)
                    lane = lanes((PITCH, 128))
                    if tiles[tile] is None:
                        tiles[tile] = block
                    else:
                        tiles[tile] = jnp.where(lane < offset, tiles[tile], block)
                    if offset + GROUP > 128:
                        tiles[tile + 1] = block
                tiles[4] = jnp.where(lanes((PITCH, 128)) < HALF - 512, tiles[4], 0.0)
                halves.append(jnp.concatenate(tiles, axis=1))
            high, low = split(jnp.concatenate(halves, axis=0))
            both = dot(jnp.concatenate([high, low], axis=0), tables[parity, :, :PAD])
            results.append(both[:80] + both[80:] + dot(high, tables[parity, :, PAD:]))
        sums = results[0] + results[1]
        differences = results[0] - results[1]
        none = jnp.zeros((80, PAD), f32)
        whole = jnp.concatenate([sums, none], axis=1) + pltpu.roll(
            jnp.concatenate([differences, none], axis=1), HALF, 1
        )
        for s in range(2):
            out_ref[s] = whole[PITCH * s : PITCH * s + ROWS, :LENGTH]
        for c in range(2):
            slab = recv2[c, 16:24]
            for e in range(2 + c, PEERS, 2):
                slab = slab + recv2[e, 16:24]
            value_ref[c] = slab

    with jax.named_scope("te_total"):
        @pl.when(core == 0)
        def _():
            over_levels(lambda e: level_from(e).wait_recv())
            total = lrecv[0]
            for e in range(1, 8):
                total = total + lrecv[e]
            tsend[...] = total * (1.0 / 16.0)
            total_to(me + 1).start()
            value_ref[2] = tsend[...]
            total_to(me + 1).wait_send()

        @pl.when(core == 1)
        def _():
            total_to(me - 1).wait_recv()
            value_ref[2] = trecv[...]

    with jax.named_scope("tf_drain"):
        over_peers(lambda e: exchange(*first_copy, e).wait_send())
        over_peers(lambda e: exchange(*second_copy, e).wait_send())
        over_heads(lambda e: energy_to(e).wait_send(), 1)

        @pl.when(core == 1)
        def _():
            energy_to(me - 1).wait_send()

        @pl.when(core == 0)
        def _():
            over_levels(lambda e: level_to(e).wait_send())


def leave_kernel(field_ref, value_ref, out_ref, energy_ref, total_ref, energies, total, sems):
    copies = [pltpu.make_async_copy(field_ref.at[s], out_ref.at[:, s], sems.at[s]) for s in range(2)]
    for copy in copies:
        copy.start()
    energies[0] = value_ref[0, 0, 124]
    energies[1] = value_ref[1, 0, 124]
    total[0] = value_ref[2, 0, 0]
    copies.append(pltpu.make_async_copy(energies, energy_ref, sems.at[2]))
    copies.append(pltpu.make_async_copy(total, total_ref, sems.at[3]))
    for copy in copies[2:]:
        copy.start()
    for copy in copies:
        copy.wait()


def local(grid_field, truncation_limit, diffusion_order, diffusion_strength, mass_weight):
    table_list = [jnp.asarray(basis(parity)) for parity in range(2)]
    vmem = pl.BlockSpec(memory_space=pltpu.VMEM)
    hbm = pl.BlockSpec(memory_space=pltpu.HBM)
    dma = pltpu.SemaphoreType.DMA
    blocks = pltpu.VMEM((PEERS, 24, 128), f32)
    word = pltpu.VMEM((8, 128), f32)
    field, values = pl.pallas_call(
        kernel,
        out_shape=(
            jax.ShapeDtypeStruct(grid_field.shape, f32),
            jax.ShapeDtypeStruct((3, 8, 128), f32),
        ),
        in_specs=[hbm] * 7,
        out_specs=(vmem, vmem),
        scratch_shapes=[
            pltpu.SMEM((LENGTH,), jnp.int32),
            pltpu.SMEM((2,), jnp.int32),
            pltpu.SMEM((2,), f32),
            pltpu.SMEM((2,), f32),
            pltpu.VMEM((2, ROWS, LENGTH), f32),
            pltpu.VMEM((2, PAD, 2 * PAD), bf16),
            pltpu.VMEM((2, PITCH, 1280), f32),
            pltpu.VMEM((80, PAD), f32),
            pltpu.VMEM((2, PAD, 128), f32),
            pltpu.VMEM((2, PAD, 128), f32),
            pltpu.VMEM((2, PAD, 128), f32),
            blocks, blocks, blocks, blocks,
            word, pltpu.VMEM((PEERS, 8, 128), f32), word, pltpu.VMEM((8, 8, 128), f32), word, word,
            dma((2,)), dma((2,)), dma((4,)), pltpu.SemaphoreType.REGULAR,
            dma((PEERS,)), dma((PEERS,)), dma((PEERS,)), dma((PEERS,)),
            dma((16,)), dma((PEERS,)), dma((8,)), dma((8,)), dma, dma,
        ],
        compiler_params=pltpu.CompilerParams(
            collective_id=0, has_side_effects=True, vmem_limit_bytes=48 * 1024 * 1024
        ),
    )(
        *[
            pltpu.with_memory_space_constraint(operand, pltpu.HBM)
            for operand in (
                jnp.transpose(grid_field, (1, 0, 2)), truncation_limit, diffusion_order,
                diffusion_strength, mass_weight, *table_list,
            )
        ]
    )
    filtered, energies, total = pl.pallas_call(
        leave_kernel,
        out_shape=(
            jax.ShapeDtypeStruct((ROWS, 2, LENGTH), f32),
            jax.ShapeDtypeStruct((2,), f32),
            jax.ShapeDtypeStruct((1,), f32),
        ),
        in_specs=[vmem, vmem],
        out_specs=(hbm, hbm, hbm),
        scratch_shapes=[pltpu.SMEM((2,), f32), pltpu.SMEM((1,), f32), dma((4,))],
        compiler_params=pltpu.CompilerParams(vmem_limit_bytes=8 * 1024 * 1024),
    )(field, values)
    return jnp.transpose(filtered, (1, 0, 2)), energies, total.reshape(())


def solution(mesh):
    placed = (P("lev", "wav", None), P(), P("lev"), P("lev"), P("lev"))
    return jax.shard_map(
        local,
        mesh=mesh,
        in_specs=placed,
        out_specs=(P("lev", "wav", None), P("lev"), P()),
        check_vma=False,
    )
```
